32 devices in a mesh: freq: 8 (over z, x), kgrp: 4 (over y, core).
Axes of the slice: x: 2, y: 2, z: 4, core: 2. Of those that a mesh axis runs over, the one named last changes fastest.
Arguments:
- hamiltonian: float32 [256, 64, 128], P(('freq', 'kgrp')), may hold values from -1 to 1, as said below
- self_energy: float32 [16, 64, 128], P('freq'), may hold values from -0.8 to 0.3, as said below
- guess_factor: float32 [16, 64, 128], P('freq'), may hold values from -0.05 to 1.25
- weights: int32 [256], replicated, may hold values from 1 to 48
- counts: int32 [16], replicated, may hold values from 1 to 3, as said below
Outputs:
- local_green: float32 [4096, 32], P(('freq', 'kgrp'))
The draws below stay inside these ranges and needn't reach their ends.
Inputs may be any that keep to these rules, and one draw needn't show every extreme that they name: `hamiltonian`: each k-point's matrix is Hermitian: the left half symmetric, the right half antisymmetric. `self_energy`: the diagonal of the right half lies between -0.8 and -0.4. `counts`: the number of Newton-Schulz steps taken at each frequency.
All inputs are finite; a program needn't handle non-finite values.
Results may differ from the reference program's by a relative error of at most 0.0001.
Values sent between devices are 32-bit elements.
A program may use at most 64 MiB of HBM per device.

```python
import math
import jax
import jax.numpy as jnp
from jax import lax

NORB = 64
MAXIT = 3
FREQ = 16
KPTS = 256


def noise_draw(key, shape, spread):
    return jax.random.truncated_normal(key, -4.0, 4.0, shape, jnp.float32) * spread


def draw_hamiltonian(key, part):
    first_key, second_key, third_key = jax.random.split(key, 3)
    identity = jnp.eye(NORB, dtype=jnp.float32)
    left_noise = noise_draw(first_key, (KPTS, NORB, NORB), 0.018)
    right_noise = noise_draw(second_key, (KPTS, NORB, NORB), 0.018)
    symmetric = (left_noise + jnp.swapaxes(left_noise, 1, 2)) * 0.70710678 * (1.0 - identity)
    skewed = (right_noise - jnp.swapaxes(right_noise, 1, 2)) * 0.70710678
    levels = jax.random.uniform(third_key, (KPTS, NORB), jnp.float32, -1.0, 1.0)
    real_part = symmetric + levels[:, :, None] * identity
    return jnp.concatenate([real_part, skewed], -1).astype(jnp.float32)


def draw_self_energy(key, part):
    first_key, second_key, third_key, fourth_key = jax.random.split(key, 4)
    identity = jnp.eye(NORB, dtype=jnp.float32)
    real_off = noise_draw(first_key, (FREQ, NORB, NORB), 0.012) * (1.0 - identity)
    imag_off = noise_draw(second_key, (FREQ, NORB, NORB), 0.012) * (1.0 - identity)
    real_diag = jax.random.uniform(third_key, (FREQ, NORB), jnp.float32, -0.3, 0.3)
    damping = jax.random.uniform(fourth_key, (FREQ, NORB), jnp.float32, -0.8, -0.4)
    real_part = real_off + real_diag[:, :, None] * identity
    imag_part = imag_off + damping[:, :, None] * identity
    return jnp.concatenate([real_part, imag_part], -1).astype(jnp.float32)


def draw_guess_factor(key, part):
    first_key, second_key, third_key = jax.random.split(key, 3)
    identity = jnp.eye(NORB, dtype=jnp.float32)
    real_off = noise_draw(first_key, (FREQ, NORB, NORB), 0.01) * (1.0 - identity)
    imag_part = noise_draw(second_key, (FREQ, NORB, NORB), 0.01)
    scales = jax.random.uniform(third_key, (FREQ, NORB), jnp.float32, 0.75, 1.25)
    real_part = real_off + scales[:, :, None] * identity
    return jnp.concatenate([real_part, imag_part], -1).astype(jnp.float32)


def draw_counts(key, part):
    positions = jnp.arange(FREQ, dtype=jnp.int32)
    extra = jax.random.randint(key, (FREQ,), 0, 4)
    lowest = (8 * positions < FREQ).astype(jnp.int32)
    bumped = ((extra == 0) & (positions < FREQ - 1)).astype(jnp.int32)
    return jnp.minimum(MAXIT, 1 + 2 * lowest + bumped).astype(jnp.int32)


def set_ends(drawn, stream_key, smallest, high):
    longest = drawn.shape.index(max(drawn.shape))
    spots = []
    for shift in (0, 1):
        where = [jax.random.randint(jax.random.fold_in(stream_key, axis), (), 0, length) for axis, length in enumerate(drawn.shape)]
        where[longest] = (where[longest] + shift) % drawn.shape[longest]
        spots.append(tuple(where))
    return drawn.at[spots[0]].set(smallest).at[spots[1]].set(high)


def setup_inputs(seed: int = 0) -> dict:
    keys = jax.random.split(jax.random.key(seed), 6)
    hamiltonian = draw_hamiltonian(jax.random.fold_in(keys[5], 71), 0)
    self_energy = draw_self_energy(jax.random.fold_in(keys[5], 71), 0)
    guess_factor = draw_guess_factor(jax.random.fold_in(keys[5], 71), 0)
    weights = set_ends(jax.random.randint(keys[3], (KPTS,), 1, 49), jax.random.fold_in(keys[3], 1), 1, 48).astype(jnp.int32)
    counts = draw_counts(jax.random.fold_in(keys[5], 71), 0)
    return dict(hamiltonian=hamiltonian, self_energy=self_energy, guess_factor=guess_factor, weights=weights, counts=counts)


chem_potential = 0.2


def blockify(right_side):
    order = right_side.shape[-1] // 2
    real_part = right_side[..., :order]
    imag_part = right_side[..., order:]
    upper_row = jnp.concatenate([real_part, imag_part], -1)
    lower_row = jnp.concatenate([-imag_part, real_part], -1)
    return jnp.concatenate([upper_row, lower_row], -2)


def complex_product(left_side, right_side):
    return jnp.einsum('...ij,...jl->...il', left_side, blockify(right_side), precision=lax.Precision.HIGHEST)


def build_matrix(kpoint_rows, sigma_rows, matsubara):
    orbitals = kpoint_rows.shape[1]
    identity = jnp.eye(orbitals, dtype=jnp.float32)
    real_shift = jnp.broadcast_to(chem_potential * identity, matsubara.shape + identity.shape)
    imag_shift = matsubara[:, None, None] * identity
    diagonal_shift = jnp.concatenate([real_shift, imag_shift], -1)
    return diagonal_shift[:, None] - kpoint_rows[None] - sigma_rows[:, None]


def start_guess(matrix, factor_rows):
    orbitals = matrix.shape[-2]
    diag_real = jnp.diagonal(matrix[..., :orbitals], axis1=-2, axis2=-1)
    diag_imag = jnp.diagonal(matrix[..., orbitals:], axis1=-2, axis2=-1)
    modulus = diag_real * diag_real + diag_imag * diag_imag
    recip_real = (diag_real / modulus)[..., None]
    recip_imag = (-diag_imag / modulus)[..., None]
    factor_real = factor_rows[..., :orbitals]
    factor_imag = factor_rows[..., orbitals:]
    guess_real = recip_real * factor_real - recip_imag * factor_imag
    guess_imag = recip_real * factor_imag + recip_imag * factor_real
    return jnp.concatenate([guess_real, guess_imag], -1)


def reference(hamiltonian, self_energy, guess_factor, weights, counts):
    orbitals = hamiltonian.shape[1]
    factors = weights.astype(jnp.float32)
    weight_total = jnp.sum(factors)
    identity = jnp.eye(orbitals, dtype=jnp.float32)
    doubled = jnp.concatenate([2.0 * identity, jnp.zeros_like(identity)], -1)

    def one_frequency(inputs):
        sigma_row, factor_row, step_count, freq_id = inputs
        matsubara = (2 * freq_id + 1).astype(jnp.float32)[None] * (math.pi / (2 * FREQ))
        matrix = build_matrix(hamiltonian, sigma_row[None], matsubara)
        initial = start_guess(matrix, factor_row[None, None])

        def newton_step(sweep, current):
            return complex_product(current, doubled - complex_product(matrix, current))

        final = lax.fori_loop(0, step_count, newton_step, initial)
        summed = jnp.einsum('k,fkij->fij', factors, final, precision=lax.Precision.HIGHEST)
        return summed[0] / weight_total

    greens = lax.map(one_frequency, (self_energy, guess_factor, counts, jnp.arange(FREQ, dtype=jnp.int32)))
    arranged = greens.reshape(FREQ, orbitals, 2, orbitals).transpose(1, 3, 2, 0)
    return arranged.reshape(orbitals * orbitals, 2 * FREQ)
```

```python
import functools
import math

import jax
import jax.numpy as jnp
from jax import lax
from jax.experimental import pallas as pl
from jax.experimental.pallas import tpu as pltpu
from jax.sharding import PartitionSpec as P

chem_potential = 0.2
MESH = pl.DeviceIdType.MESH
VMEM = pl.BlockSpec(memory_space=pltpu.VMEM)
SMEM = pl.BlockSpec(memory_space=pltpu.SMEM)


def split(value):
    high = value.astype(jnp.bfloat16).astype(jnp.float32)
    return high, value - high


def left_operand(value, half, left):
    high, low = split(value)
    turned_high, turned_low = split(pltpu.roll(value, half, 1))
    top = jnp.where(left, high, turned_low)
    bottom = jnp.where(left, turned_high, low)
    return jnp.concatenate([top, bottom], 0).astype(jnp.bfloat16)


def right_operand(value):
    high, low = split(value)
    row = jnp.concatenate([high, low], 1).astype(jnp.bfloat16)
    return jnp.concatenate([row, row], 0)


def fold(product, orbitals, sign):
    width = 2 * orbitals
    both = product[:, :width] + product[:, width:]
    return both[:orbitals] + sign * pltpu.roll(both[orbitals:], orbitals, 1)


def invert_kernel(
    counts, weights, h_ref, sigma_ref, guess_ref, out_ref, m_left, x_now, h_diag, last_left, last_right
):
    k_local, orbitals, width = h_ref.shape
    freq_total = sigma_ref.shape[0]
    shape = (orbitals, width)
    row = lax.broadcasted_iota(jnp.int32, shape, 0)
    lane = lax.broadcasted_iota(jnp.int32, shape, 1)
    left = lane < orbitals
    sign = jnp.where(left, -1.0, 1.0)
    eye_real = (lane == row).astype(jnp.float32)
    eye_imag = (lane == row + orbitals).astype(jnp.float32)
    device = lax.axis_index("freq") * lax.axis_size("kgrp") + lax.axis_index("kgrp")

    def add_weight(index, total):
        return total + weights[index]

    weight_total = lax.fori_loop(
        0, weights.shape[0], add_weight, jnp.int32(0), unroll=8
    ).astype(jnp.float32)
    factors = [
        jnp.full((1, width), weights[device * k_local + k].astype(jnp.float32)) / weight_total
        for k in range(k_local)
    ]

    def diagonal(value):
        real = jnp.sum(value * eye_real, axis=1, keepdims=True)
        imag = jnp.sum(value * eye_imag, axis=1, keepdims=True)
        return jnp.broadcast_to(real, shape), jnp.broadcast_to(imag, shape)

    for k in range(k_local):
        h_diag[0, k], h_diag[1, k] = diagonal(h_ref[k])

    def one_frequency(freq, carry):
        matsubara = (2 * freq + 1).astype(jnp.float32) * (math.pi / (2 * freq_total))
        base = (chem_potential * eye_real + matsubara * eye_imag) - sigma_ref[freq]
        base_real, base_imag = diagonal(base)
        guess = guess_ref[freq]
        turned = sign * pltpu.roll(guess, orbitals, 1)
        for k in range(k_local):
            matrix = base - h_ref[k]
            m_left[k] = left_operand(matrix, orbitals, left)
            real = base_real - h_diag[0, k]
            imag = base_imag - h_diag[1, k]
            inverse = 1.0 / (real * real + imag * imag)
            x_now[k] = (real * inverse) * guess - (imag * inverse) * turned

        def residual(k, current):
            product = jnp.dot(
                m_left[k], right_operand(current), preferred_element_type=jnp.float32
            )
            return eye_real - fold(product, orbitals, sign)

        def newton_step(sweep, inner):
            for k in range(k_local):
                current = x_now[k]
                missing = residual(k, current)
                product = jnp.dot(
                    left_operand(current, orbitals, left),
                    right_operand(missing),
                    preferred_element_type=jnp.float32,
                )
                x_now[k] = current + fold(product, orbitals, sign)
            return inner

        lax.fori_loop(0, counts[freq] - 1, newton_step, 0)
        total = jnp.zeros(shape, jnp.float32)
        for k in range(k_local):
            current = x_now[k]
            last_right[k * width : (k + 1) * width, :] = right_operand(residual(k, current))
            weighted = current * factors[k]
            last_left[:, k * width : (k + 1) * width] = left_operand(weighted, orbitals, left)
            total = total + weighted
        product = jnp.dot(last_left[...], last_right[...], preferred_element_type=jnp.float32)
        total = total + fold(product, orbitals, sign)
        out_ref[pl.ds(freq, orbitals, stride=freq_total), :] = total
        return carry

    lax.fori_loop(0, freq_total, one_frequency, 0)


def invert(counts, weights, hamiltonian, sigma, guess):
    k_local, orbitals, width = hamiltonian.shape
    freq_total = sigma.shape[0]
    return pl.pallas_call(
        invert_kernel,
        out_shape=jax.ShapeDtypeStruct((orbitals * freq_total, width), jnp.float32),
        in_specs=[SMEM, SMEM, VMEM, VMEM, VMEM],
        out_specs=VMEM,
        scratch_shapes=[
            pltpu.VMEM((k_local, width, width), jnp.bfloat16),
            pltpu.VMEM((k_local, orbitals, width), jnp.float32),
            pltpu.VMEM((2, k_local, orbitals, width), jnp.float32),
            pltpu.VMEM((width, k_local * width), jnp.bfloat16),
            pltpu.VMEM((k_local * width, 2 * width), jnp.bfloat16),
        ],
        name="invert",
    )(counts, weights, hamiltonian, sigma, guess)


def gather_kernel(sigma_ref, guess_ref, out_sigma, out_guess, local_sem, send, recv, pass_send, pass_recv):
    per_freq = sigma_ref.shape[0]
    freq_devs = lax.axis_size("freq")
    me = lax.axis_index("freq")
    group = lax.axis_index("kgrp")
    parity = lax.rem(group, 2)
    mate = group + 1 - 2 * parity
    barrier = pltpu.get_barrier_semaphore()
    for shift in range(1, freq_devs):
        pl.semaphore_signal(
            barrier, inc=1, device_id=(lax.rem(me + shift, freq_devs), group), device_id_type=MESH
        )
    pl.semaphore_signal(barrier, inc=1, device_id=(me, mate), device_id_type=MESH)
    own = pl.ds(me * per_freq, per_freq)
    keeps = [
        pltpu.make_async_copy(sigma_ref, out_sigma.at[own], local_sem.at[0]),
        pltpu.make_async_copy(guess_ref, out_guess.at[own], local_sem.at[1]),
    ]
    for keep in keeps:
        keep.start()
    pl.semaphore_wait(barrier, freq_devs)

    def exchange(source, target):
        copies = []
        for shift in range(1, freq_devs):
            copies.append(
                pltpu.make_async_remote_copy(
                    src_ref=source,
                    dst_ref=target.at[own],
                    send_sem=send.at[shift],
                    recv_sem=recv.at[shift],
                    device_id=(lax.rem(me + shift, freq_devs), group),
                    device_id_type=MESH,
                )
            )
        for copy in copies:
            copy.start()
        passes = []
        for shift in range(1, freq_devs):
            copies[shift - 1].wait_recv()
            origin = lax.rem(me - shift + freq_devs, freq_devs)
            landed = target.at[pl.ds(origin * per_freq, per_freq)]
            forward = pltpu.make_async_remote_copy(
                src_ref=landed,
                dst_ref=landed,
                send_sem=pass_send.at[shift],
                recv_sem=pass_recv.at[shift],
                device_id=(me, mate),
                device_id_type=MESH,
            )
            forward.start()
            passes.append(forward)
        for forward in passes:
            forward.wait()
        for copy in copies:
            copy.wait_send()

    @pl.when(parity == 0)
    def _():
        exchange(sigma_ref, out_sigma)

    @pl.when(parity == 1)
    def _():
        exchange(guess_ref, out_guess)

    for keep in keeps:
        keep.wait()


def gather(self_energy, guess_factor, freq_devs):
    per_freq, orbitals, width = self_energy.shape
    full = jax.ShapeDtypeStruct((per_freq * freq_devs, orbitals, width), jnp.float32)
    return pl.pallas_call(
        gather_kernel,
        out_shape=(full, full),
        in_specs=[VMEM, VMEM],
        out_specs=(VMEM, VMEM),
        scratch_shapes=[
            pltpu.SemaphoreType.DMA((2,)),
            pltpu.SemaphoreType.DMA((freq_devs,)),
            pltpu.SemaphoreType.DMA((freq_devs,)),
            pltpu.SemaphoreType.DMA((freq_devs,)),
            pltpu.SemaphoreType.DMA((freq_devs,)),
        ],
        compiler_params=pltpu.CompilerParams(collective_id=0, has_side_effects=True),
        name="gather",
    )(self_energy, guess_factor)


def scatter_kernel(part_ref, out_ref, mate_half, summed, landed, mate_sems, send, recv):
    freq_devs, pairs, _, rows, width = part_ref.shape
    me = lax.axis_index("freq")
    group = lax.axis_index("kgrp")
    half = group // 2
    parity = lax.rem(group, 2)
    mate = group + 1 - 2 * parity
    others = [(a, b) for a in range(freq_devs) for b in range(pairs) if a + b > 0]
    barrier = pltpu.get_barrier_semaphore()

    def place(step, back=False):
        a, b = step
        if back:
            a, b = freq_devs - a, pairs - b
        return lax.rem(me + a, freq_devs), lax.rem(half + b, pairs)

    for step in others:
        freq_to, half_to = place(step)
        pl.semaphore_signal(
            barrier, inc=1, device_id=(freq_to, 2 * half_to + parity), device_id_type=MESH
        )
    pl.semaphore_signal(barrier, inc=1, device_id=(me, mate), device_id_type=MESH)
    pl.semaphore_wait(barrier, len(others) + 1)
    swaps = []
    for freq_to in range(freq_devs):
        swap = pltpu.make_async_remote_copy(
            src_ref=part_ref.at[freq_to, :, 1 - parity],
            dst_ref=mate_half.at[freq_to],
            send_sem=mate_sems.at[0, freq_to],
            recv_sem=mate_sems.at[1, freq_to],
            device_id=(me, mate),
            device_id_type=MESH,
        )
        swap.start()
        swaps.append(swap)
    for freq_to in range(freq_devs):
        swaps[freq_to].wait_recv()
        for half_to in range(pairs):
            summed[freq_to, half_to] = (
                part_ref[freq_to, half_to, parity] + mate_half[freq_to, half_to]
            )
    copies = []
    for index, step in enumerate(others):
        freq_to, half_to = place(step)
        copy = pltpu.make_async_remote_copy(
            src_ref=summed.at[freq_to, half_to],
            dst_ref=landed.at[index],
            send_sem=send.at[index],
            recv_sem=recv.at[index],
            device_id=(freq_to, 2 * half_to + parity),
            device_id_type=MESH,
        )
        copy.start()
        copies.append(copy)
    total = summed[me, half]
    for index, copy in enumerate(copies):
        copy.wait_recv()
        total = total + landed[index]
    out_ref[...] = total
    for copy in copies:
        copy.wait_send()
    for swap in swaps:
        swap.wait_send()


def scatter(partial, freq_devs, group_devs):
    rows, width = partial.shape
    pairs = group_devs // 2
    own_rows = rows // (freq_devs * group_devs)
    peers = freq_devs * pairs - 1
    block = (own_rows, width)
    return pl.pallas_call(
        scatter_kernel,
        out_shape=jax.ShapeDtypeStruct(block, jnp.float32),
        in_specs=[VMEM],
        out_specs=VMEM,
        scratch_shapes=[
            pltpu.VMEM((freq_devs, pairs) + block, jnp.float32),
            pltpu.VMEM((freq_devs, pairs) + block, jnp.float32),
            pltpu.VMEM((peers,) + block, jnp.float32),
            pltpu.SemaphoreType.DMA((2, freq_devs)),
            pltpu.SemaphoreType.DMA((peers,)),
            pltpu.SemaphoreType.DMA((peers,)),
        ],
        compiler_params=pltpu.CompilerParams(collective_id=1, has_side_effects=True),
        name="scatter",
    )(partial.reshape(freq_devs, pairs, 2, own_rows, width))


def per_device(hamiltonian, self_energy, guess_factor, weights, counts):
    orbitals = hamiltonian.shape[1]
    per_freq = self_energy.shape[0]
    freq_devs = lax.axis_size("freq")
    group_devs = lax.axis_size("kgrp")
    freq_total = per_freq * freq_devs
    pair_block = orbitals * orbitals // (freq_devs * group_devs)
    direct = pair_block % orbitals == 0 and group_devs % 2 == 0
    if direct:
        sigma, guess = gather(self_energy, guess_factor, freq_devs)
    else:
        sigma = lax.all_gather(self_energy, "freq", axis=0, tiled=True)
        guess = lax.all_gather(guess_factor, "freq", axis=0, tiled=True)
    partial = invert(counts, weights, hamiltonian, sigma, guess)
    if direct:
        own = scatter(partial, freq_devs, group_devs)
        own = own.reshape(pair_block // orbitals, freq_total, 2, orbitals)
        result = own.transpose(0, 3, 2, 1)
    else:
        terms = partial.reshape(orbitals, freq_total, 2, orbitals).transpose(0, 3, 2, 1)
        terms = terms.reshape(orbitals * orbitals, 2 * freq_total)
        result = lax.psum_scatter(terms, ("freq", "kgrp"), scatter_dimension=0, tiled=True)
    return result.reshape(pair_block, 2 * freq_total)


def solution(mesh):
    return jax.shard_map(
        per_device,
        mesh=mesh,
        in_specs=(
            P(("freq", "kgrp"), None, None),
            P("freq", None, None),
            P("freq", None, None),
            P(),
            P(),
        ),
        out_specs=P(("freq", "kgrp"), None),
        check_vma=False,
    )
```

```python
import functools
import math

import jax
import jax.numpy as jnp
from jax import lax
from jax.experimental import pallas as pl
from jax.experimental.pallas import tpu as pltpu
from jax.sharding import PartitionSpec as P

chem_potential = 0.2
MESH = pl.DeviceIdType.MESH
VMEM = pl.BlockSpec(memory_space=pltpu.VMEM)
SMEM = pl.BlockSpec(memory_space=pltpu.SMEM)


def split(value):
    high = value.astype(jnp.bfloat16).astype(jnp.float32)
    return high, value - high


def left_operand(value, half, left):
    high, low = split(value)
    turned_high, turned_low = split(pltpu.roll(value, half, 1))
    top = jnp.where(left, high, turned_low)
    bottom = jnp.where(left, turned_high, low)
    return jnp.concatenate([top, bottom], 0).astype(jnp.bfloat16)


def right_operand(value):
    high, low = split(value)
    row = jnp.concatenate([high, low], 1).astype(jnp.bfloat16)
    return jnp.concatenate([row, row], 0)


def fold(product, orbitals, sign):
    width = 2 * orbitals
    both = product[:, :width] + product[:, width:]
    return both[:orbitals] + sign * pltpu.roll(both[orbitals:], orbitals, 1)


def masks(shape):
    orbitals = shape[0]
    row = lax.broadcasted_iota(jnp.int32, shape, 0)
    lane = lax.broadcasted_iota(jnp.int32, shape, 1)
    left = lane < orbitals
    sign = jnp.where(left, -1.0, 1.0)
    eye_real = (lane == row).astype(jnp.float32)
    eye_imag = (lane == row + orbitals).astype(jnp.float32)
    return left, sign, eye_real, eye_imag


def shifted(freq, freq_total, eye_real, eye_imag, sigma):
    matsubara = (2 * freq + 1).astype(jnp.float32) * (math.pi / (2 * freq_total))
    return (chem_potential * eye_real + matsubara * eye_imag) - sigma


def steps_kernel(counts, weights, h_ref, sigma_ref, guess_ref, x_ref, factor_ref, m_left, h_diag):
    k_local, orbitals, width = h_ref.shape
    freq_total = sigma_ref.shape[0]
    shape = (orbitals, width)
    left, sign, eye_real, eye_imag = masks(shape)
    device = lax.axis_index("freq") * lax.axis_size("kgrp") + lax.axis_index("kgrp")

    def add_weight(index, total):
        return total + weights[index]

    weight_total = lax.fori_loop(
        0, weights.shape[0], add_weight, jnp.int32(0), unroll=8
    ).astype(jnp.float32)
    for k in range(k_local):
        weight = weights[device * k_local + k].astype(jnp.float32)
        factor_ref[k : k + 1, :] = jnp.full((1, width), weight) / weight_total

    def diagonal(value):
        real = jnp.sum(value * eye_real, axis=1, keepdims=True)
        imag = jnp.sum(value * eye_imag, axis=1, keepdims=True)
        return jnp.broadcast_to(real, shape), jnp.broadcast_to(imag, shape)

    for k in range(k_local):
        h_diag[0, k], h_diag[1, k] = diagonal(h_ref[k])

    def one_frequency(freq, carry):
        base = shifted(freq, freq_total, eye_real, eye_imag, sigma_ref[freq])
        base_real, base_imag = diagonal(base)
        guess = guess_ref[freq]
        turned = sign * pltpu.roll(guess, orbitals, 1)
        for k in range(k_local):
            real = base_real - h_diag[0, k]
            imag = base_imag - h_diag[1, k]
            inverse = 1.0 / (real * real + imag * imag)
            x_ref[freq, k] = (real * inverse) * guess - (imag * inverse) * turned

        @pl.when(counts[freq] > 1)
        def _():
            for k in range(k_local):
                m_left[k] = left_operand(base - h_ref[k], orbitals, left)

            def newton_step(sweep, inner):
                for k in range(k_local):
                    current = x_ref[freq, k]
                    product = jnp.dot(
                        m_left[k], right_operand(current), preferred_element_type=jnp.float32
                    )
                    missing = eye_real - fold(product, orbitals, sign)
                    product = jnp.dot(
                        left_operand(current, orbitals, left),
                        right_operand(missing),
                        preferred_element_type=jnp.float32,
                    )
                    x_ref[freq, k] = current + fold(product, orbitals, sign)
                return inner

            lax.fori_loop(0, counts[freq] - 1, newton_step, 0)

        return carry

    lax.fori_loop(0, freq_total, one_frequency, 0)


def early_steps(counts, weights, hamiltonian, sigma, guess):
    k_local, orbitals, width = hamiltonian.shape
    freq_total = sigma.shape[0]
    return pl.pallas_call(
        steps_kernel,
        out_shape=(
            jax.ShapeDtypeStruct((freq_total, k_local, orbitals, width), jnp.float32),
            jax.ShapeDtypeStruct((k_local, width), jnp.float32),
        ),
        in_specs=[SMEM, SMEM, VMEM, VMEM, VMEM],
        out_specs=(VMEM, VMEM),
        scratch_shapes=[
            pltpu.VMEM((k_local, width, width), jnp.bfloat16),
            pltpu.VMEM((2, k_local, orbitals, width), jnp.float32),
        ],
        name="early_steps",
    )(counts, weights, hamiltonian, sigma, guess)


def last_step(freq, freq_total, factor_ref, h_ref, sigma_ref, x_ref, last_left, last_right):
    k_local, orbitals, width = h_ref.shape
    left, sign, eye_real, eye_imag = masks((orbitals, width))
    base = shifted(freq, freq_total, eye_real, eye_imag, sigma_ref[freq])
    total = jnp.zeros((orbitals, width), jnp.float32)
    for k in range(k_local):
        current = x_ref[freq, k]
        product = jnp.dot(
            left_operand(base - h_ref[k], orbitals, left),
            right_operand(current),
            preferred_element_type=jnp.float32,
        )
        missing = eye_real - fold(product, orbitals, sign)
        last_right[k * width : (k + 1) * width, :] = right_operand(missing)
        weighted = current * factor_ref[k : k + 1, :]
        last_left[:, k * width : (k + 1) * width] = left_operand(weighted, orbitals, left)
        total = total + weighted
    product = jnp.dot(last_left[...], last_right[...], preferred_element_type=jnp.float32)
    return total + fold(product, orbitals, sign)


def last_scratch(k_local, width):
    return [
        pltpu.VMEM((width, k_local * width), jnp.bfloat16),
        pltpu.VMEM((k_local * width, 2 * width), jnp.bfloat16),
    ]


def sum_kernel(factor_ref, h_ref, sigma_ref, x_ref, out_ref, last_left, last_right):
    freq_total = sigma_ref.shape[0]

    def one_frequency(freq, carry):
        out_ref[freq] = last_step(
            freq, freq_total, factor_ref, h_ref, sigma_ref, x_ref, last_left, last_right
        )
        return carry

    lax.fori_loop(0, freq_total, one_frequency, 0)


def local_sum(factors, hamiltonian, sigma, current):
    k_local, orbitals, width = hamiltonian.shape
    return pl.pallas_call(
        sum_kernel,
        out_shape=jax.ShapeDtypeStruct(sigma.shape, jnp.float32),
        in_specs=[VMEM] * 4,
        out_specs=VMEM,
        scratch_shapes=last_scratch(k_local, width),
        name="local_sum",
    )(factors, hamiltonian, sigma, current)


def gather_kernel(
    sigma_ref, guess_ref, out_sigma, out_guess, local_sem, send, recv, side_send, side_recv, pass_send, pass_recv
):
    per_freq = sigma_ref.shape[0]
    freq_devs = lax.axis_size("freq")
    column = freq_devs // 2
    me = lax.axis_index("freq")
    group = lax.axis_index("kgrp")
    parity = lax.rem(group, 2)
    mate = group + 1 - 2 * parity
    beside = me + 1 - 2 * lax.rem(me, 2)
    barrier = pltpu.get_barrier_semaphore()
    for shift in range(1, column):
        pl.semaphore_signal(
            barrier, inc=1, device_id=(lax.rem(me + 2 * shift, freq_devs), group), device_id_type=MESH
        )
    pl.semaphore_signal(barrier, inc=1, device_id=(beside, group), device_id_type=MESH)
    pl.semaphore_signal(barrier, inc=1, device_id=(me, mate), device_id_type=MESH)
    own = pl.ds(me * per_freq, per_freq)
    keeps = [
        pltpu.make_async_copy(sigma_ref, out_sigma.at[own], local_sem.at[0]),
        pltpu.make_async_copy(guess_ref, out_guess.at[own], local_sem.at[1]),
    ]
    for keep in keeps:
        keep.start()
    pl.semaphore_wait(barrier, column + 1)

    def exchange(source, target):
        def piece(origin):
            return target.at[pl.ds(origin * per_freq, per_freq)]

        def remote(src, dst, send_sem, recv_sem, freq_to, group_to):
            copy = pltpu.make_async_remote_copy(
                src_ref=src,
                dst_ref=dst,
                send_sem=send_sem,
                recv_sem=recv_sem,
                device_id=(freq_to, group_to),
                device_id_type=MESH,
            )
            copy.start()
            return copy

        along = {}
        for shift in range(1, column):
            freq_to = lax.rem(me + 2 * shift, freq_devs)
            along[shift] = remote(
                source, piece(me), send.at[shift], recv.at[shift], freq_to, group
            )
        across = [remote(source, piece(me), side_send.at[0], side_recv.at[0], beside, group)]
        passes = []

        def hand(origin):
            slot = len(passes)
            landed = piece(origin)
            passes.append(
                remote(landed, landed, pass_send.at[slot], pass_recv.at[slot], me, mate)
            )

        for shift in range(1, column):
            along[shift].wait_recv()
            origin = lax.rem(me - 2 * shift + freq_devs, freq_devs)
            landed = piece(origin)
            across.append(
                remote(landed, landed, side_send.at[shift], side_recv.at[shift], beside, group)
            )
            hand(origin)
        for shift in range(column):
            across[shift].wait_recv()
            hand(lax.rem(beside - 2 * shift + freq_devs, freq_devs))
        for copy in passes:
            copy.wait()
        for copy in list(along.values()) + across:
            copy.wait_send()

    @pl.when(parity == 0)
    def _():
        exchange(sigma_ref, out_sigma)

    @pl.when(parity == 1)
    def _():
        exchange(guess_ref, out_guess)

    for keep in keeps:
        keep.wait()


def gather(self_energy, guess_factor, freq_devs):
    per_freq, orbitals, width = self_energy.shape
    full = jax.ShapeDtypeStruct((per_freq * freq_devs, orbitals, width), jnp.float32)
    sems = pltpu.SemaphoreType.DMA((freq_devs,))
    return pl.pallas_call(
        gather_kernel,
        out_shape=(full, full),
        in_specs=[VMEM, VMEM],
        out_specs=(VMEM, VMEM),
        scratch_shapes=[pltpu.SemaphoreType.DMA((2,))] + [sems] * 6,
        compiler_params=pltpu.CompilerParams(collective_id=0, has_side_effects=True),
        name="gather",
    )(self_energy, guess_factor)


def scatter_kernel(
    factor_ref,
    h_ref,
    sigma_ref,
    x_ref,
    out_ref,
    last_left,
    last_right,
    part,
    mate_half,
    summed,
    landed,
    mate_send,
    mate_recv,
    send,
    recv,
):
    chunks, freq_devs, pairs, _, rows, width = part.shape
    orbitals = h_ref.shape[1]
    freq_total = sigma_ref.shape[0]
    per_chunk = freq_total // chunks
    me = lax.axis_index("freq")
    group = lax.axis_index("kgrp")
    half = group // 2
    parity = lax.rem(group, 2)
    mate = group + 1 - 2 * parity
    others = [(a, b) for a in range(freq_devs) for b in range(pairs) if a + b > 0]
    barrier = pltpu.get_barrier_semaphore()
    flat = part.reshape(chunks, orbitals * per_chunk, width)

    def place(step):
        return lax.rem(me + step[0], freq_devs), lax.rem(half + step[1], pairs)

    for step in others:
        freq_to, half_to = place(step)
        pl.semaphore_signal(
            barrier, inc=1, device_id=(freq_to, 2 * half_to + parity), device_id_type=MESH
        )
    pl.semaphore_signal(barrier, inc=1, device_id=(me, mate), device_id_type=MESH)

    def swap(chunk):
        return pltpu.make_async_remote_copy(
            src_ref=part.at[chunk, :, :, 1 - parity],
            dst_ref=mate_half.at[chunk],
            send_sem=mate_send.at[chunk],
            recv_sem=mate_recv.at[chunk],
            device_id=(me, mate),
            device_id_type=MESH,
        )

    def spread(chunk, index):
        freq_to, half_to = place(others[index])
        return pltpu.make_async_remote_copy(
            src_ref=summed.at[chunk, freq_to, half_to],
            dst_ref=landed.at[chunk, index],
            send_sem=send.at[chunk, index],
            recv_sem=recv.at[chunk, index],
            device_id=(freq_to, 2 * half_to + parity),
            device_id_type=MESH,
        )

    def forward(chunk):
        swap(chunk).wait_recv()
        for freq_to in range(freq_devs):
            for half_to in range(pairs):
                summed[chunk, freq_to, half_to] = (
                    part[chunk, freq_to, half_to, parity] + mate_half[chunk, freq_to, half_to]
                )
        for index in range(len(others)):
            spread(chunk, index).start()

    def one_chunk(chunk, carry):
        def one_frequency(index, inner):
            flat[chunk, pl.ds(index, orbitals, stride=per_chunk), :] = last_step(
                chunk * per_chunk + index,
                freq_total,
                factor_ref,
                h_ref,
                sigma_ref,
                x_ref,
                last_left,
                last_right,
            )
            return inner

        lax.fori_loop(0, per_chunk, one_frequency, 0)

        @pl.when(chunk == 0)
        def _():
            pl.semaphore_wait(barrier, len(others) + 1)

        swap(chunk).start()

        @pl.when(chunk > 0)
        def _():
            forward(chunk - 1)

        return carry

    lax.fori_loop(0, chunks, one_chunk, 0)
    forward(chunks - 1)
    for chunk in range(chunks):
        total = summed[chunk, me, half]
        for index in range(len(others)):
            spread(chunk, index).wait_recv()
            total = total + landed[chunk, index]
        out_ref[chunk] = total
    for chunk in range(chunks):
        for index in range(len(others)):
            spread(chunk, index).wait_send()
        swap(chunk).wait_send()


def scatter(factors, hamiltonian, sigma, current, freq_devs, group_devs, chunks):
    k_local, orbitals, width = hamiltonian.shape
    freq_total = sigma.shape[0]
    pairs = group_devs // 2
    rows = orbitals * freq_total // (chunks * freq_devs * group_devs)
    peers = freq_devs * pairs - 1
    block = (rows, width)
    return pl.pallas_call(
        scatter_kernel,
        out_shape=jax.ShapeDtypeStruct((chunks,) + block, jnp.float32),
        in_specs=[VMEM] * 4,
        out_specs=VMEM,
        scratch_shapes=last_scratch(k_local, width)
        + [
            pltpu.VMEM((chunks, freq_devs, pairs, 2) + block, jnp.float32),
            pltpu.VMEM((chunks, freq_devs, pairs) + block, jnp.float32),
            pltpu.VMEM((chunks, freq_devs, pairs) + block, jnp.float32),
            pltpu.VMEM((chunks, peers) + block, jnp.float32),
            pltpu.SemaphoreType.DMA((chunks,)),
            pltpu.SemaphoreType.DMA((chunks,)),
            pltpu.SemaphoreType.DMA((chunks, peers)),
            pltpu.SemaphoreType.DMA((chunks, peers)),
        ],
        compiler_params=pltpu.CompilerParams(collective_id=1, has_side_effects=True),
        name="scatter",
    )(factors, hamiltonian, sigma, current)


def per_device(hamiltonian, self_energy, guess_factor, weights, counts):
    orbitals = hamiltonian.shape[1]
    per_freq = self_energy.shape[0]
    freq_devs = lax.axis_size("freq")
    group_devs = lax.axis_size("kgrp")
    freq_total = per_freq * freq_devs
    pair_block = orbitals * orbitals // (freq_devs * group_devs)
    pair_rows = pair_block // orbitals
    direct = pair_block % orbitals == 0 and group_devs % 2 == 0 and freq_devs % 2 == 0
    per_chunk = 8 // pair_rows if direct and 8 % pair_rows == 0 else freq_total
    direct = direct and freq_total % per_chunk == 0 and (pair_rows * per_chunk) % 8 == 0
    if direct:
        sigma, guess = gather(self_energy, guess_factor, freq_devs)
    else:
        sigma = lax.all_gather(self_energy, "freq", axis=0, tiled=True)
        guess = lax.all_gather(guess_factor, "freq", axis=0, tiled=True)
    current, factors = early_steps(counts, weights, hamiltonian, sigma, guess)
    if direct:
        chunks = freq_total // per_chunk
        own = scatter(factors, hamiltonian, sigma, current, freq_devs, group_devs, chunks)
        own = own.reshape(chunks, pair_rows, per_chunk, 2, orbitals)
        result = own.transpose(1, 4, 3, 0, 2)
    else:
        terms = local_sum(factors, hamiltonian, sigma, current)
        terms = terms.reshape(freq_total, orbitals, 2, orbitals).transpose(1, 3, 2, 0)
        terms = terms.reshape(orbitals * orbitals, 2 * freq_total)
        result = lax.psum_scatter(terms, ("freq", "kgrp"), scatter_dimension=0, tiled=True)
    return result.reshape(pair_block, 2 * freq_total)


def solution(mesh):
    return jax.shard_map(
        per_device,
        mesh=mesh,
        in_specs=(
            P(("freq", "kgrp"), None, None),
            P("freq", None, None),
            P("freq", None, None),
            P(),
            P(),
        ),
        out_specs=P(("freq", "kgrp"), None),
        check_vma=False,
    )
```

```python
import functools
import math

import jax
import jax.numpy as jnp
from jax import lax
from jax.experimental import pallas as pl
from jax.experimental.pallas import tpu as pltpu
from jax.sharding import PartitionSpec as P

chem_potential = 0.2
MESH = pl.DeviceIdType.MESH
VMEM = pl.BlockSpec(memory_space=pltpu.VMEM)
SMEM = pl.BlockSpec(memory_space=pltpu.SMEM)


def split(value):
    high = value.astype(jnp.bfloat16).astype(jnp.float32)
    return high, value - high


def left_operand(value, half, left):
    high, low = split(value)
    turned_high, turned_low = split(pltpu.roll(value, half, 1))
    top = jnp.where(left, high, turned_low)
    bottom = jnp.where(left, turned_high, low)
    return jnp.concatenate([top, bottom], 0).astype(jnp.bfloat16)


def right_operand(value):
    high, low = split(value)
    row = jnp.concatenate([high, low], 1).astype(jnp.bfloat16)
    return jnp.concatenate([row, row], 0)


def fold(product, orbitals, sign):
    width = 2 * orbitals
    both = product[:, :width] + product[:, width:]
    return both[:orbitals] + sign * pltpu.roll(both[orbitals:], orbitals, 1)


def masks(shape):
    orbitals = shape[0]
    row = lax.broadcasted_iota(jnp.int32, shape, 0)
    lane = lax.broadcasted_iota(jnp.int32, shape, 1)
    left = lane < orbitals
    sign = jnp.where(left, -1.0, 1.0)
    eye_real = (lane == row).astype(jnp.float32)
    eye_imag = (lane == row + orbitals).astype(jnp.float32)
    return left, sign, eye_real, eye_imag


def shifted(freq, freq_total, eye_real, eye_imag, sigma):
    matsubara = (2 * freq + 1).astype(jnp.float32) * (math.pi / (2 * freq_total))
    return (chem_potential * eye_real + matsubara * eye_imag) - sigma


def steps_kernel(counts, weights, h_ref, sigma_ref, guess_ref, x_ref, factor_ref, m_left, h_diag):
    k_local, orbitals, width = h_ref.shape
    freq_total = sigma_ref.shape[0]
    shape = (orbitals, width)
    left, sign, eye_real, eye_imag = masks(shape)
    device = lax.axis_index("freq") * lax.axis_size("kgrp") + lax.axis_index("kgrp")

    def add_weight(index, total):
        return total + weights[index]

    weight_total = lax.fori_loop(
        0, weights.shape[0], add_weight, jnp.int32(0), unroll=8
    ).astype(jnp.float32)
    for k in range(k_local):
        weight = weights[device * k_local + k].astype(jnp.float32)
        factor_ref[k : k + 1, :] = jnp.full((1, width), weight) / weight_total

    def diagonal(value):
        real = jnp.sum(value * eye_real, axis=1, keepdims=True)
        imag = jnp.sum(value * eye_imag, axis=1, keepdims=True)
        return jnp.broadcast_to(real, shape), jnp.broadcast_to(imag, shape)

    for k in range(k_local):
        h_diag[0, k], h_diag[1, k] = diagonal(h_ref[k])

    def one_frequency(freq, carry):
        base = shifted(freq, freq_total, eye_real, eye_imag, sigma_ref[freq])
        base_real, base_imag = diagonal(base)
        guess = guess_ref[freq]
        turned = sign * pltpu.roll(guess, orbitals, 1)
        for k in range(k_local):
            real = base_real - h_diag[0, k]
            imag = base_imag - h_diag[1, k]
            inverse = 1.0 / (real * real + imag * imag)
            x_ref[freq, k] = (real * inverse) * guess - (imag * inverse) * turned

        @pl.when(counts[freq] > 1)
        def _():
            for k in range(k_local):
                m_left[k] = left_operand(base - h_ref[k], orbitals, left)

            def newton_step(sweep, inner):
                products = [
                    jnp.dot(
                        m_left[k],
                        right_operand(x_ref[freq, k]),
                        preferred_element_type=jnp.float32,
                    )
                    for k in range(k_local)
                ]
                products = [
                    jnp.dot(
                        left_operand(x_ref[freq, k], orbitals, left),
                        right_operand(eye_real - fold(products[k], orbitals, sign)),
                        preferred_element_type=jnp.float32,
                    )
                    for k in range(k_local)
                ]
                for k in range(k_local):
                    x_ref[freq, k] = x_ref[freq, k] + fold(products[k], orbitals, sign)
                return inner

            lax.fori_loop(0, counts[freq] - 1, newton_step, 0)

        return carry

    lax.fori_loop(0, freq_total, one_frequency, 0)


def early_steps(counts, weights, hamiltonian, sigma, guess):
    k_local, orbitals, width = hamiltonian.shape
    freq_total = sigma.shape[0]
    return pl.pallas_call(
        steps_kernel,
        out_shape=(
            jax.ShapeDtypeStruct((freq_total, k_local, orbitals, width), jnp.float32),
            jax.ShapeDtypeStruct((k_local, width), jnp.float32),
        ),
        in_specs=[SMEM, SMEM, VMEM, VMEM, VMEM],
        out_specs=(VMEM, VMEM),
        scratch_shapes=[
            pltpu.VMEM((k_local, width, width), jnp.bfloat16),
            pltpu.VMEM((2, k_local, orbitals, width), jnp.float32),
        ],
        name="early_steps",
    )(counts, weights, hamiltonian, sigma, guess)


def last_step(freq, freq_total, factor_ref, h_ref, sigma_ref, x_ref, last_left, last_right):
    k_local, orbitals, width = h_ref.shape
    left, sign, eye_real, eye_imag = masks((orbitals, width))
    base = shifted(freq, freq_total, eye_real, eye_imag, sigma_ref[freq])
    products = [
        jnp.dot(
            left_operand(base - h_ref[k], orbitals, left),
            right_operand(x_ref[freq, k]),
            preferred_element_type=jnp.float32,
        )
        for k in range(k_local)
    ]
    total = jnp.zeros((orbitals, width), jnp.float32)
    for k in range(k_local):
        weighted = x_ref[freq, k] * factor_ref[k : k + 1, :]
        last_left[:, k * width : (k + 1) * width] = left_operand(weighted, orbitals, left)
        total = total + weighted
    for k in range(k_local):
        missing = eye_real - fold(products[k], orbitals, sign)
        last_right[k * width : (k + 1) * width, :] = right_operand(missing)
    product = jnp.dot(last_left[...], last_right[...], preferred_element_type=jnp.float32)
    return total + fold(product, orbitals, sign)


def last_scratch(k_local, width):
    return [
        pltpu.VMEM((width, k_local * width), jnp.bfloat16),
        pltpu.VMEM((k_local * width, 2 * width), jnp.bfloat16),
    ]


def sum_kernel(factor_ref, h_ref, sigma_ref, x_ref, out_ref, last_left, last_right):
    freq_total = sigma_ref.shape[0]

    def one_frequency(freq, carry):
        out_ref[freq] = last_step(
            freq, freq_total, factor_ref, h_ref, sigma_ref, x_ref, last_left, last_right
        )
        return carry

    lax.fori_loop(0, freq_total, one_frequency, 0)


def local_sum(factors, hamiltonian, sigma, current):
    k_local, orbitals, width = hamiltonian.shape
    return pl.pallas_call(
        sum_kernel,
        out_shape=jax.ShapeDtypeStruct(sigma.shape, jnp.float32),
        in_specs=[VMEM] * 4,
        out_specs=VMEM,
        scratch_shapes=last_scratch(k_local, width),
        name="local_sum",
    )(factors, hamiltonian, sigma, current)


def gather_kernel(
    sigma_ref, guess_ref, out_sigma, out_guess, local_sem, send, recv, side_send, side_recv, pass_send, pass_recv
):
    per_freq = sigma_ref.shape[0]
    freq_devs = lax.axis_size("freq")
    column = freq_devs // 2
    me = lax.axis_index("freq")
    group = lax.axis_index("kgrp")
    parity = lax.rem(group, 2)
    mate = group + 1 - 2 * parity
    beside = me + 1 - 2 * lax.rem(me, 2)
    barrier = pltpu.get_barrier_semaphore()
    for shift in range(1, column):
        pl.semaphore_signal(
            barrier, inc=1, device_id=(lax.rem(me + 2 * shift, freq_devs), group), device_id_type=MESH
        )
    pl.semaphore_signal(barrier, inc=1, device_id=(beside, group), device_id_type=MESH)
    pl.semaphore_signal(barrier, inc=1, device_id=(me, mate), device_id_type=MESH)
    own = pl.ds(me * per_freq, per_freq)
    keeps = [
        pltpu.make_async_copy(sigma_ref, out_sigma.at[own], local_sem.at[0]),
        pltpu.make_async_copy(guess_ref, out_guess.at[own], local_sem.at[1]),
    ]
    for keep in keeps:
        keep.start()
    pl.semaphore_wait(barrier, column + 1)

    def exchange(source, target):
        def piece(origin):
            return target.at[pl.ds(origin * per_freq, per_freq)]

        def remote(src, dst, send_sem, recv_sem, freq_to, group_to):
            copy = pltpu.make_async_remote_copy(
                src_ref=src,
                dst_ref=dst,
                send_sem=send_sem,
                recv_sem=recv_sem,
                device_id=(freq_to, group_to),
                device_id_type=MESH,
            )
            copy.start()
            return copy

        along = {}
        for shift in range(1, column):
            freq_to = lax.rem(me + 2 * shift, freq_devs)
            along[shift] = remote(
                source, piece(me), send.at[shift], recv.at[shift], freq_to, group
            )
        across = [remote(source, piece(me), side_send.at[0], side_recv.at[0], beside, group)]
        passes = []

        def hand(origin):
            slot = len(passes)
            landed = piece(origin)
            passes.append(
                remote(landed, landed, pass_send.at[slot], pass_recv.at[slot], me, mate)
            )

        for shift in range(1, column):
            along[shift].wait_recv()
            origin = lax.rem(me - 2 * shift + freq_devs, freq_devs)
            landed = piece(origin)
            across.append(
                remote(landed, landed, side_send.at[shift], side_recv.at[shift], beside, group)
            )
            hand(origin)
        for shift in range(column):
            across[shift].wait_recv()
            hand(lax.rem(beside - 2 * shift + freq_devs, freq_devs))
        for copy in passes:
            copy.wait()
        for copy in list(along.values()) + across:
            copy.wait_send()

    @pl.when(parity == 0)
    def _():
        exchange(sigma_ref, out_sigma)

    @pl.when(parity == 1)
    def _():
        exchange(guess_ref, out_guess)

    for keep in keeps:
        keep.wait()


def gather(self_energy, guess_factor, freq_devs):
    per_freq, orbitals, width = self_energy.shape
    full = jax.ShapeDtypeStruct((per_freq * freq_devs, orbitals, width), jnp.float32)
    sems = pltpu.SemaphoreType.DMA((freq_devs,))
    return pl.pallas_call(
        gather_kernel,
        out_shape=(full, full),
        in_specs=[VMEM, VMEM],
        out_specs=(VMEM, VMEM),
        scratch_shapes=[pltpu.SemaphoreType.DMA((2,))] + [sems] * 6,
        compiler_params=pltpu.CompilerParams(collective_id=0, has_side_effects=True),
        name="gather",
    )(self_energy, guess_factor)


def scatter_kernel(
    factor_ref,
    h_ref,
    sigma_ref,
    x_ref,
    out_ref,
    last_left,
    last_right,
    part,
    mate_half,
    summed,
    landed,
    mate_send,
    mate_recv,
    send,
    recv,
):
    chunks, freq_devs, pairs, _, rows, width = part.shape
    orbitals = h_ref.shape[1]
    freq_total = sigma_ref.shape[0]
    per_chunk = freq_total // chunks
    me = lax.axis_index("freq")
    group = lax.axis_index("kgrp")
    half = group // 2
    parity = lax.rem(group, 2)
    mate = group + 1 - 2 * parity
    others = [(a, b) for a in range(freq_devs) for b in range(pairs) if a + b > 0]
    barrier = pltpu.get_barrier_semaphore()
    flat = part.reshape(chunks, orbitals * per_chunk, width)

    def place(step):
        return lax.rem(me + step[0], freq_devs), lax.rem(half + step[1], pairs)

    for step in others:
        freq_to, half_to = place(step)
        pl.semaphore_signal(
            barrier, inc=1, device_id=(freq_to, 2 * half_to + parity), device_id_type=MESH
        )
    pl.semaphore_signal(barrier, inc=1, device_id=(me, mate), device_id_type=MESH)

    def swap(chunk):
        return pltpu.make_async_remote_copy(
            src_ref=part.at[chunk, :, :, 1 - parity],
            dst_ref=mate_half.at[chunk],
            send_sem=mate_send.at[chunk],
            recv_sem=mate_recv.at[chunk],
            device_id=(me, mate),
            device_id_type=MESH,
        )

    def spread(chunk, index):
        freq_to, half_to = place(others[index])
        return pltpu.make_async_remote_copy(
            src_ref=summed.at[chunk, freq_to, half_to],
            dst_ref=landed.at[chunk, index],
            send_sem=send.at[chunk, index],
            recv_sem=recv.at[chunk, index],
            device_id=(freq_to, 2 * half_to + parity),
            device_id_type=MESH,
        )

    def forward(chunk):
        swap(chunk).wait_recv()
        for freq_to in range(freq_devs):
            for half_to in range(pairs):
                summed[chunk, freq_to, half_to] = (
                    part[chunk, freq_to, half_to, parity] + mate_half[chunk, freq_to, half_to]
                )
        for index in range(len(others)):
            spread(chunk, index).start()

    def one_chunk(chunk, carry):
        def one_frequency(index, inner):
            flat[chunk, pl.ds(index, orbitals, stride=per_chunk), :] = last_step(
                chunk * per_chunk + index,
                freq_total,
                factor_ref,
                h_ref,
                sigma_ref,
                x_ref,
                last_left,
                last_right,
            )
            return inner

        lax.fori_loop(0, per_chunk, one_frequency, 0)

        @pl.when(chunk == 0)
        def _():
            pl.semaphore_wait(barrier, len(others) + 1)

        swap(chunk).start()

        @pl.when(chunk > 0)
        def _():
            forward(chunk - 1)

        return carry

    lax.fori_loop(0, chunks, one_chunk, 0)
    forward(chunks - 1)
    for chunk in range(chunks):
        total = summed[chunk, me, half]
        for index in range(len(others)):
            spread(chunk, index).wait_recv()
            total = total + landed[chunk, index]
        out_ref[chunk] = total
    for chunk in range(chunks):
        for index in range(len(others)):
            spread(chunk, index).wait_send()
        swap(chunk).wait_send()


def scatter(factors, hamiltonian, sigma, current, freq_devs, group_devs, chunks):
    k_local, orbitals, width = hamiltonian.shape
    freq_total = sigma.shape[0]
    pairs = group_devs // 2
    rows = orbitals * freq_total // (chunks * freq_devs * group_devs)
    peers = freq_devs * pairs - 1
    block = (rows, width)
    return pl.pallas_call(
        scatter_kernel,
        out_shape=jax.ShapeDtypeStruct((chunks,) + block, jnp.float32),
        in_specs=[VMEM] * 4,
        out_specs=VMEM,
        scratch_shapes=last_scratch(k_local, width)
        + [
            pltpu.VMEM((chunks, freq_devs, pairs, 2) + block, jnp.float32),
            pltpu.VMEM((chunks, freq_devs, pairs) + block, jnp.float32),
            pltpu.VMEM((chunks, freq_devs, pairs) + block, jnp.float32),
            pltpu.VMEM((chunks, peers) + block, jnp.float32),
            pltpu.SemaphoreType.DMA((chunks,)),
            pltpu.SemaphoreType.DMA((chunks,)),
            pltpu.SemaphoreType.DMA((chunks, peers)),
            pltpu.SemaphoreType.DMA((chunks, peers)),
        ],
        compiler_params=pltpu.CompilerParams(collective_id=1, has_side_effects=True),
        name="scatter",
    )(factors, hamiltonian, sigma, current)


def per_device(hamiltonian, self_energy, guess_factor, weights, counts):
    orbitals = hamiltonian.shape[1]
    per_freq = self_energy.shape[0]
    freq_devs = lax.axis_size("freq")
    group_devs = lax.axis_size("kgrp")
    freq_total = per_freq * freq_devs
    pair_block = orbitals * orbitals // (freq_devs * group_devs)
    pair_rows = pair_block // orbitals
    direct = pair_block % orbitals == 0 and group_devs % 2 == 0 and freq_devs % 2 == 0
    per_chunk = 8 // pair_rows if direct and 8 % pair_rows == 0 else freq_total
    direct = direct and freq_total % per_chunk == 0 and (pair_rows * per_chunk) % 8 == 0
    if direct:
        sigma, guess = gather(self_energy, guess_factor, freq_devs)
    else:
        sigma = lax.all_gather(self_energy, "freq", axis=0, tiled=True)
        guess = lax.all_gather(guess_factor, "freq", axis=0, tiled=True)
    current, factors = early_steps(counts, weights, hamiltonian, sigma, guess)
    if direct:
        chunks = freq_total // per_chunk
        own = scatter(factors, hamiltonian, sigma, current, freq_devs, group_devs, chunks)
        own = own.reshape(chunks, pair_rows, per_chunk, 2, orbitals)
        result = own.transpose(1, 4, 3, 0, 2)
    else:
        terms = local_sum(factors, hamiltonian, sigma, current)
        terms = terms.reshape(freq_total, orbitals, 2, orbitals).transpose(1, 3, 2, 0)
        terms = terms.reshape(orbitals * orbitals, 2 * freq_total)
        result = lax.psum_scatter(terms, ("freq", "kgrp"), scatter_dimension=0, tiled=True)
    return result.reshape(pair_block, 2 * freq_total)


def solution(mesh):
    return jax.shard_map(
        per_device,
        mesh=mesh,
        in_specs=(
            P(("freq", "kgrp"), None, None),
            P("freq", None, None),
            P("freq", None, None),
            P(),
            P(),
        ),
        out_specs=P(("freq", "kgrp"), None),
        check_vma=False,
    )
```

```python
import functools
import math

import jax
import jax.numpy as jnp
from jax import lax
from jax.experimental import pallas as pl
from jax.experimental.pallas import tpu as pltpu
from jax.sharding import PartitionSpec as P

chem_potential = 0.2
MESH = pl.DeviceIdType.MESH
GRANT = 32 * 1024 * 1024
VMEM = pl.BlockSpec(memory_space=pltpu.VMEM)
SMEM = pl.BlockSpec(memory_space=pltpu.SMEM)


def split(value):
    high = value.astype(jnp.bfloat16).astype(jnp.float32)
    return high, value - high


def left_operand(value, half, left):
    high, low = split(value)
    turned_high, turned_low = split(pltpu.roll(value, half, 1))
    top = jnp.where(left, high, turned_low)
    bottom = jnp.where(left, turned_high, low)
    return jnp.concatenate([top, bottom], 0).astype(jnp.bfloat16)


def right_operand(value):
    high, low = split(value)
    row = jnp.concatenate([high, low], 1).astype(jnp.bfloat16)
    return jnp.concatenate([row, row], 0)


def fold(product, orbitals, sign):
    width = 2 * orbitals
    both = product[:, :width] + product[:, width:]
    return both[:orbitals] + sign * pltpu.roll(both[orbitals:], orbitals, 1)


def masks(shape):
    orbitals = shape[0]
    row = lax.broadcasted_iota(jnp.int32, shape, 0)
    lane = lax.broadcasted_iota(jnp.int32, shape, 1)
    left = lane < orbitals
    sign = jnp.where(left, -1.0, 1.0)
    eye_real = (lane == row).astype(jnp.float32)
    eye_imag = (lane == row + orbitals).astype(jnp.float32)
    return left, sign, eye_real, eye_imag


def shifted(freq, freq_total, eye_real, eye_imag, sigma):
    matsubara = (2 * freq + 1).astype(jnp.float32) * (math.pi / (2 * freq_total))
    return (chem_potential * eye_real + matsubara * eye_imag) - sigma


def steps_kernel(counts, weights, h_ref, sigma_ref, guess_ref, x_ref, factor_ref, m_left, h_diag):
    k_local, orbitals, width = h_ref.shape
    freq_total = sigma_ref.shape[0]
    shape = (orbitals, width)
    left, sign, eye_real, eye_imag = masks(shape)
    device = lax.axis_index("freq") * lax.axis_size("kgrp") + lax.axis_index("kgrp")

    def add_weight(index, total):
        return total + weights[index]

    weight_total = lax.fori_loop(
        0, weights.shape[0], add_weight, jnp.int32(0), unroll=8
    ).astype(jnp.float32)
    for k in range(k_local):
        weight = weights[device * k_local + k].astype(jnp.float32)
        factor_ref[k : k + 1, :] = jnp.full((1, width), weight) / weight_total

    def diagonal(value):
        real = jnp.sum(value * eye_real, axis=1, keepdims=True)
        imag = jnp.sum(value * eye_imag, axis=1, keepdims=True)
        return jnp.broadcast_to(real, shape), jnp.broadcast_to(imag, shape)

    for k in range(k_local):
        h_diag[0, k], h_diag[1, k] = diagonal(h_ref[k])

    def one_frequency(freq, carry):
        base = shifted(freq, freq_total, eye_real, eye_imag, sigma_ref[freq])
        base_real, base_imag = diagonal(base)
        guess = guess_ref[freq]
        turned = sign * pltpu.roll(guess, orbitals, 1)
        for k in range(k_local):
            real = base_real - h_diag[0, k]
            imag = base_imag - h_diag[1, k]
            inverse = 1.0 / (real * real + imag * imag)
            x_ref[freq, k] = (real * inverse) * guess - (imag * inverse) * turned

        @pl.when(counts[freq] > 1)
        def _():
            for k in range(k_local):
                m_left[k] = left_operand(base - h_ref[k], orbitals, left)

            def newton_step(sweep, inner):
                products = [
                    jnp.dot(
                        m_left[k],
                        right_operand(x_ref[freq, k]),
                        preferred_element_type=jnp.float32,
                    )
                    for k in range(k_local)
                ]
                products = [
                    jnp.dot(
                        left_operand(x_ref[freq, k], orbitals, left),
                        right_operand(eye_real - fold(products[k], orbitals, sign)),
                        preferred_element_type=jnp.float32,
                    )
                    for k in range(k_local)
                ]
                for k in range(k_local):
                    x_ref[freq, k] = x_ref[freq, k] + fold(products[k], orbitals, sign)
                return inner

            lax.fori_loop(0, counts[freq] - 1, newton_step, 0)

        return carry

    lax.fori_loop(0, freq_total, one_frequency, 0)


def early_steps(counts, weights, hamiltonian, sigma, guess):
    k_local, orbitals, width = hamiltonian.shape
    freq_total = sigma.shape[0]
    return pl.pallas_call(
        steps_kernel,
        out_shape=(
            jax.ShapeDtypeStruct((freq_total, k_local, orbitals, width), jnp.float32),
            jax.ShapeDtypeStruct((k_local, width), jnp.float32),
        ),
        in_specs=[SMEM, SMEM, VMEM, VMEM, VMEM],
        out_specs=(VMEM, VMEM),
        scratch_shapes=[
            pltpu.VMEM((k_local, width, width), jnp.bfloat16),
            pltpu.VMEM((2, k_local, orbitals, width), jnp.float32),
        ],
        compiler_params=pltpu.CompilerParams(vmem_limit_bytes=GRANT),
        name="early_steps",
    )(counts, weights, hamiltonian, sigma, guess)


def last_step(freq, freq_total, factor_ref, h_ref, sigma_ref, x_ref, last_left, last_right):
    k_local, orbitals, width = h_ref.shape
    left, sign, eye_real, eye_imag = masks((orbitals, width))
    base = shifted(freq, freq_total, eye_real, eye_imag, sigma_ref[freq])
    products = [
        jnp.dot(
            left_operand(base - h_ref[k], orbitals, left),
            right_operand(x_ref[freq, k]),
            preferred_element_type=jnp.float32,
        )
        for k in range(k_local)
    ]
    total = jnp.zeros((orbitals, width), jnp.float32)
    for k in range(k_local):
        weighted = x_ref[freq, k] * factor_ref[k : k + 1, :]
        last_left[:, k * width : (k + 1) * width] = left_operand(weighted, orbitals, left)
        total = total + weighted
    for k in range(k_local):
        missing = eye_real - fold(products[k], orbitals, sign)
        last_right[k * width : (k + 1) * width, :] = right_operand(missing)
    product = jnp.dot(last_left[...], last_right[...], preferred_element_type=jnp.float32)
    return total + fold(product, orbitals, sign)


def last_scratch(k_local, width):
    return [
        pltpu.VMEM((width, k_local * width), jnp.bfloat16),
        pltpu.VMEM((k_local * width, 2 * width), jnp.bfloat16),
    ]


def sum_kernel(factor_ref, h_ref, sigma_ref, x_ref, out_ref, last_left, last_right):
    freq_total = sigma_ref.shape[0]

    def one_frequency(freq, carry):
        out_ref[freq] = last_step(
            freq, freq_total, factor_ref, h_ref, sigma_ref, x_ref, last_left, last_right
        )
        return carry

    lax.fori_loop(0, freq_total, one_frequency, 0)


def local_sum(factors, hamiltonian, sigma, current):
    k_local, orbitals, width = hamiltonian.shape
    return pl.pallas_call(
        sum_kernel,
        out_shape=jax.ShapeDtypeStruct(sigma.shape, jnp.float32),
        in_specs=[VMEM] * 4,
        out_specs=VMEM,
        scratch_shapes=last_scratch(k_local, width),
        name="local_sum",
    )(factors, hamiltonian, sigma, current)


def gather_kernel(
    sigma_ref, guess_ref, out_sigma, out_guess, local_sem, send, recv, side_send, side_recv, pass_send, pass_recv
):
    per_freq = sigma_ref.shape[0]
    freq_devs = lax.axis_size("freq")
    column = freq_devs // 2
    me = lax.axis_index("freq")
    group = lax.axis_index("kgrp")
    parity = lax.rem(group, 2)
    mate = group + 1 - 2 * parity
    beside = me + 1 - 2 * lax.rem(me, 2)
    barrier = pltpu.get_barrier_semaphore()
    for shift in range(1, column):
        pl.semaphore_signal(
            barrier, inc=1, device_id=(lax.rem(me + 2 * shift, freq_devs), group), device_id_type=MESH
        )
    pl.semaphore_signal(barrier, inc=1, device_id=(beside, group), device_id_type=MESH)
    pl.semaphore_signal(barrier, inc=1, device_id=(me, mate), device_id_type=MESH)
    own = pl.ds(me * per_freq, per_freq)
    keeps = [
        pltpu.make_async_copy(sigma_ref, out_sigma.at[own], local_sem.at[0]),
        pltpu.make_async_copy(guess_ref, out_guess.at[own], local_sem.at[1]),
    ]
    for keep in keeps:
        keep.start()
    pl.semaphore_wait(barrier, column + 1)

    def exchange(source, target):
        def piece(origin):
            return target.at[pl.ds(origin * per_freq, per_freq)]

        def remote(src, dst, send_sem, recv_sem, freq_to, group_to):
            copy = pltpu.make_async_remote_copy(
                src_ref=src,
                dst_ref=dst,
                send_sem=send_sem,
                recv_sem=recv_sem,
                device_id=(freq_to, group_to),
                device_id_type=MESH,
            )
            copy.start()
            return copy

        along = {}
        for shift in range(1, column):
            freq_to = lax.rem(me + 2 * shift, freq_devs)
            along[shift] = remote(
                source, piece(me), send.at[shift], recv.at[shift], freq_to, group
            )
        across = [remote(source, piece(me), side_send.at[0], side_recv.at[0], beside, group)]
        passes = []

        def hand(origin):
            slot = len(passes)
            landed = piece(origin)
            passes.append(
                remote(landed, landed, pass_send.at[slot], pass_recv.at[slot], me, mate)
            )

        for shift in range(1, column):
            along[shift].wait_recv()
            origin = lax.rem(me - 2 * shift + freq_devs, freq_devs)
            landed = piece(origin)
            across.append(
                remote(landed, landed, side_send.at[shift], side_recv.at[shift], beside, group)
            )
            hand(origin)
        for shift in range(column):
            across[shift].wait_recv()
            hand(lax.rem(beside - 2 * shift + freq_devs, freq_devs))
        for copy in passes:
            copy.wait()
        for copy in list(along.values()) + across:
            copy.wait_send()

    @pl.when(parity == 0)
    def _():
        exchange(sigma_ref, out_sigma)

    @pl.when(parity == 1)
    def _():
        exchange(guess_ref, out_guess)

    for keep in keeps:
        keep.wait()


def gather(self_energy, guess_factor, freq_devs):
    per_freq, orbitals, width = self_energy.shape
    full = jax.ShapeDtypeStruct((per_freq * freq_devs, orbitals, width), jnp.float32)
    sems = pltpu.SemaphoreType.DMA((freq_devs,))
    return pl.pallas_call(
        gather_kernel,
        out_shape=(full, full),
        in_specs=[VMEM, VMEM],
        out_specs=(VMEM, VMEM),
        scratch_shapes=[pltpu.SemaphoreType.DMA((2,))] + [sems] * 6,
        compiler_params=pltpu.CompilerParams(collective_id=0, has_side_effects=True, vmem_limit_bytes=GRANT),
        name="gather",
    )(self_energy, guess_factor)


def scatter_kernel(
    factor_ref,
    h_ref,
    sigma_ref,
    x_ref,
    out_ref,
    last_left,
    last_right,
    part,
    mate_half,
    summed,
    landed,
    mate_send,
    mate_recv,
    send,
    recv,
):
    chunks, freq_devs, pairs, _, rows, width = part.shape
    orbitals = h_ref.shape[1]
    freq_total = sigma_ref.shape[0]
    per_chunk = freq_total // chunks
    me = lax.axis_index("freq")
    group = lax.axis_index("kgrp")
    half = group // 2
    parity = lax.rem(group, 2)
    mate = group + 1 - 2 * parity
    others = [(a, b) for a in range(freq_devs) for b in range(pairs) if a + b > 0]
    barrier = pltpu.get_barrier_semaphore()
    flat = part.reshape(chunks, orbitals * per_chunk, width)

    def place(step):
        return lax.rem(me + step[0], freq_devs), lax.rem(half + step[1], pairs)

    for step in others:
        freq_to, half_to = place(step)
        pl.semaphore_signal(
            barrier, inc=1, device_id=(freq_to, 2 * half_to + parity), device_id_type=MESH
        )
    pl.semaphore_signal(barrier, inc=1, device_id=(me, mate), device_id_type=MESH)

    def swap(chunk):
        return pltpu.make_async_remote_copy(
            src_ref=part.at[chunk, :, :, 1 - parity],
            dst_ref=mate_half.at[chunk],
            send_sem=mate_send.at[chunk],
            recv_sem=mate_recv.at[chunk],
            device_id=(me, mate),
            device_id_type=MESH,
        )

    def spread(chunk, index):
        freq_to, half_to = place(others[index])
        return pltpu.make_async_remote_copy(
            src_ref=summed.at[chunk, freq_to, half_to],
            dst_ref=landed.at[chunk, index],
            send_sem=send.at[chunk, index],
            recv_sem=recv.at[chunk, index],
            device_id=(freq_to, 2 * half_to + parity),
            device_id_type=MESH,
        )

    def forward(chunk):
        swap(chunk).wait_recv()
        for freq_to in range(freq_devs):
            for half_to in range(pairs):
                summed[chunk, freq_to, half_to] = (
                    part[chunk, freq_to, half_to, parity] + mate_half[chunk, freq_to, half_to]
                )
        for index in range(len(others)):
            spread(chunk, index).start()

    def one_chunk(chunk, carry):
        def one_frequency(index, inner):
            flat[chunk, pl.ds(index, orbitals, stride=per_chunk), :] = last_step(
                chunk * per_chunk + index,
                freq_total,
                factor_ref,
                h_ref,
                sigma_ref,
                x_ref,
                last_left,
                last_right,
            )
            return inner

        lax.fori_loop(0, per_chunk, one_frequency, 0)

        @pl.when(chunk == 0)
        def _():
            pl.semaphore_wait(barrier, len(others) + 1)

        swap(chunk).start()

        @pl.when(chunk > 0)
        def _():
            forward(chunk - 1)

        return carry

    lax.fori_loop(0, chunks, one_chunk, 0)
    forward(chunks - 1)
    for chunk in range(chunks):
        total = summed[chunk, me, half]
        for index in range(len(others)):
            spread(chunk, index).wait_recv()
            total = total + landed[chunk, index]
        out_ref[chunk] = total
    for chunk in range(chunks):
        for index in range(len(others)):
            spread(chunk, index).wait_send()
        swap(chunk).wait_send()


def scatter(factors, hamiltonian, sigma, current, freq_devs, group_devs, chunks):
    k_local, orbitals, width = hamiltonian.shape
    freq_total = sigma.shape[0]
    pairs = group_devs // 2
    rows = orbitals * freq_total // (chunks * freq_devs * group_devs)
    peers = freq_devs * pairs - 1
    block = (rows, width)
    return pl.pallas_call(
        scatter_kernel,
        out_shape=jax.ShapeDtypeStruct((chunks,) + block, jnp.float32),
        in_specs=[VMEM] * 4,
        out_specs=VMEM,
        scratch_shapes=last_scratch(k_local, width)
        + [
            pltpu.VMEM((chunks, freq_devs, pairs, 2) + block, jnp.float32),
            pltpu.VMEM((chunks, freq_devs, pairs) + block, jnp.float32),
            pltpu.VMEM((chunks, freq_devs, pairs) + block, jnp.float32),
            pltpu.VMEM((chunks, peers) + block, jnp.float32),
            pltpu.SemaphoreType.DMA((chunks,)),
            pltpu.SemaphoreType.DMA((chunks,)),
            pltpu.SemaphoreType.DMA((chunks, peers)),
            pltpu.SemaphoreType.DMA((chunks, peers)),
        ],
        compiler_params=pltpu.CompilerParams(collective_id=1, has_side_effects=True, vmem_limit_bytes=GRANT),
        name="scatter",
    )(factors, hamiltonian, sigma, current)


def per_device(hamiltonian, self_energy, guess_factor, weights, counts):
    orbitals = hamiltonian.shape[1]
    per_freq = self_energy.shape[0]
    freq_devs = lax.axis_size("freq")
    group_devs = lax.axis_size("kgrp")
    freq_total = per_freq * freq_devs
    pair_block = orbitals * orbitals // (freq_devs * group_devs)
    pair_rows = pair_block // orbitals
    direct = pair_block % orbitals == 0 and group_devs % 2 == 0 and freq_devs % 2 == 0
    per_chunk = 8 // pair_rows if direct and 8 % pair_rows == 0 else freq_total
    direct = direct and freq_total % per_chunk == 0 and (pair_rows * per_chunk) % 8 == 0
    if direct:
        sigma, guess = gather(self_energy, guess_factor, freq_devs)
    else:
        sigma = lax.all_gather(self_energy, "freq", axis=0, tiled=True)
        guess = lax.all_gather(guess_factor, "freq", axis=0, tiled=True)
    current, factors = early_steps(counts, weights, hamiltonian, sigma, guess)
    if direct:
        chunks = freq_total // per_chunk
        own = scatter(factors, hamiltonian, sigma, current, freq_devs, group_devs, chunks)
        own = own.reshape(chunks, pair_rows, per_chunk, 2, orbitals)
        result = own.transpose(1, 4, 3, 0, 2)
    else:
        terms = local_sum(factors, hamiltonian, sigma, current)
        terms = terms.reshape(freq_total, orbitals, 2, orbitals).transpose(1, 3, 2, 0)
        terms = terms.reshape(orbitals * orbitals, 2 * freq_total)
        result = lax.psum_scatter(terms, ("freq", "kgrp"), scatter_dimension=0, tiled=True)
    return result.reshape(pair_block, 2 * freq_total)


def solution(mesh):
    return jax.shard_map(
        per_device,
        mesh=mesh,
        in_specs=(
            P(("freq", "kgrp"), None, None),
            P("freq", None, None),
            P("freq", None, None),
            P(),
            P(),
        ),
        out_specs=P(("freq", "kgrp"), None),
        check_vma=False,
    )
```
